1024 devices in a mesh: rows: 16 (over y, x), mp: 64 (over z, core).
Axes of the slice: x: 4, y: 4, z: 32, core: 2. Of those that a mesh axis runs over, the one named last changes fastest.
Arguments:
- tokens: bfloat16 [2048, 6144], P('rows', 'mp'), may hold values from -8 to 8
- norm_gain: float32 [6144], replicated, may hold values from 0.25 to 1.75
- hidden_bias: float32 [24576], P('mp'), may hold values from -3 to 3
- weight_in: bfloat16 [6144, 24576], P('rows', 'mp'), may hold values from -0.078125 to 0.078125
- weight_out: bfloat16 [24576, 6144], P('mp', 'rows'), may hold values from -0.109375 to 0.109375
Outputs:
- updated: bfloat16 [2048, 6144], P('rows', 'mp')
The draws below stay inside these ranges and needn't reach their ends.
All inputs are finite; a program needn't handle non-finite values.
Results may differ from the reference program's by a relative error of at most 0.0041.
Values may be sent and summed in bfloat16 or wider, within the bound.
A program may use at most 64 MiB of HBM per device.

```python
import jax
import jax.numpy as jnp
from jax import lax

D = 6144
FF = 24576
TOKENS = 2048


def raised(array, own_key, source, target, blocks, factor):
    owner, partner = [(jnp.arange(array.shape[position]) // (array.shape[position] // blocks)).reshape([-1 if axis == position else 1 for axis in range(array.ndim)]) for position in (source, target)]
    chosen = jax.random.permutation(own_key, blocks)[partner]
    strong = (owner == chosen) | (owner == (partner + blocks // 2) % blocks)
    return jnp.where(strong, factor * array, array)


def block_scale(own_key, extent, cuts, smallest, high):
    factor_of = 1.0
    for dim, blocks in cuts:
        heights = jax.random.uniform(jax.random.fold_in(jax.random.fold_in(own_key, 6), dim), (blocks,), jnp.float32, smallest / len(cuts), high / len(cuts))
        factor_of = factor_of * jnp.repeat(jnp.exp(heights), extent[dim] // blocks).reshape((-1,) + (1,) * (len(extent) - 1 - dim))
    return factor_of


def gaussian(own_key, extent, spread, limit, split=(), dtype=jnp.bfloat16):
    array = spread * jax.random.normal(own_key, extent, jnp.float32)
    if split:
        array = array * block_scale(own_key, extent, split, -0.22, 0.18)
    return jnp.clip(array, -limit, limit).astype(dtype)


def heavy_noise(stream_key, extent, spread, reach, shards, heavy, kind=jnp.bfloat16):
    array = spread * jax.random.normal(stream_key, extent, jnp.float32)
    if shards:
        array = array * block_scale(stream_key, extent, shards, -0.22, 0.18)
    return jnp.clip(raised(array, jax.random.fold_in(stream_key, 3), *heavy), -reach, reach).astype(kind)


def setup_inputs(seed: int = 0) -> dict:
    streams_of = jax.random.split(jax.random.key(seed), 6)
    return {
        "tokens": heavy_noise(streams_of[0], (TOKENS, D), 1.0, 8.0, ((0, 16), (1, 64)), (1, 0, 64, 4.0)),
        "norm_gain": jnp.clip(1.0 + 0.15 * jax.random.normal(streams_of[1], (D,), jnp.float32), 0.25, 1.75),
        "hidden_bias": gaussian(streams_of[2], (FF,), 0.5, 3.0, ((0, 64),), jnp.float32),
        "weight_in": gaussian(streams_of[3], (D, FF), D ** -0.5, 0.078125, ((0, 16), (1, 64))),
        "weight_out": heavy_noise(streams_of[4], (FF, D), FF ** -0.5, 0.109375, ((0, 64), (1, 16)), (0, 1, 64, 4.0)),
    }


floor_value = 0.1

def normalize(as_float, moment_sum, square_sum, gain, width):
    row_mean = moment_sum / width
    row_var = jnp.maximum(square_sum / width - row_mean * row_mean, 0.0)
    inverse = lax.rsqrt(row_var + floor_value)
    return ((as_float - row_mean[:, None]) * inverse[:, None] * gain[None, :]).astype(jnp.bfloat16)

def reference(tokens, norm_gain, hidden_bias, weight_in, weight_out):
    as_float = tokens.astype(jnp.float32)
    normed = normalize(as_float, lax.optimization_barrier(jnp.sum(as_float, axis=1)), lax.optimization_barrier(jnp.sum(as_float * as_float, axis=1)), norm_gain, D)
    preact = jnp.dot(normed, weight_in, preferred_element_type=jnp.float32) + hidden_bias[None, :]
    hidden = jax.nn.gelu(preact, approximate=False).astype(jnp.bfloat16)
    branch = jnp.dot(hidden, weight_out, preferred_element_type=jnp.float32)
    return (as_float + branch).astype(jnp.bfloat16)
```

```python
import jax
import jax.numpy as jnp
from jax import lax
from jax.experimental import pallas as pl
from jax.experimental.pallas import tpu as pltpu
from jax.sharding import Mesh
from jax.sharding import PartitionSpec as P

MP = ("mp_0", "mp_1")
ROWS = ("rows_0", "rows_1")
NZ = 32
NP = 4
NR = 16
TOK = 128
FEAT = 96
BLK = 384
HALF = 192
WIDTH = NZ * 2 * FEAT
STEPS = NZ // 2
F32 = jnp.float32
BF16 = jnp.bfloat16

floor_value = 0.1


def gelu(v):
    return 0.5 * v * (1.0 + lax.erf(v * 0.7071067811865476))


def kernel(
    tok_ref, gain_ref, bias_ref, win_ref, wout_ref, out_ref,
    xt, nx, w1, w2, gt, hid, pad, rsin, rsout, res, part,
    ag_send, ag_recv, push_send, own_send, own_recv,
    pl_send, pl_recv, wp_send, wp_recv, nb_send, nb_recv,
    hid_send, hid_recv, rs_send, rs_recv, res_send, res_recv,
):
    y = lax.axis_index("rows_0")
    x = lax.axis_index("rows_1")
    z = lax.axis_index("mp_0")
    c = lax.axis_index("mp_1")
    r = y * NP + x

    def dev(yy, xx, zz, cc):
        return (yy, xx, zz, cc)

    partner = dev(y, x, z, 1 - c)
    zup = dev(y, x, (z + 1) % NZ, c)
    zdn = dev(y, x, (z + NZ - 1) % NZ, c)

    def remote(src, dst, ssem, rsem, to):
        return pltpu.make_async_remote_copy(
            src_ref=src, dst_ref=dst, send_sem=ssem, recv_sem=rsem,
            device_id=to, device_id_type=pl.DeviceIdType.MESH,
        )

    def signal_all(targets):
        bar = pltpu.get_barrier_semaphore()
        for t in targets:
            pl.semaphore_signal(bar, inc=1, device_id=t, device_id_type=pl.DeviceIdType.MESH)

    def wait_all(n):
        pl.semaphore_wait(pltpu.get_barrier_semaphore(), n)

    xup = dev(y, (x + 1) % NP, z, c)
    xdn = dev(y, (x + NP - 1) % NP, z, c)
    yup = dev((y + 1) % NP, x, z, c)
    ydn = dev((y + NP - 1) % NP, x, z, c)

    @pl.when(c == 0)
    def _():
        signal_all([partner, xup, xdn, yup, ydn])

    @pl.when(c == 1)
    def _():
        signal_all([partner, zup, zdn])

    pad[...] = jnp.zeros((128, 128), F32)
    pad[:, 0:FEAT] = tok_ref[...].astype(F32)
    xt[z, c] = pad[...].T[0:FEAT, :].astype(BF16)

    def put_weight(src, dst):
        t = src[...].astype(F32).T.astype(BF16)
        dst[c, 2 * r] = t[0:HALF, :]
        dst[c, 2 * r + 1] = t[HALF:BLK, :]

    def spread_gain(t):
        row = gain_ref[pl.ds(t, 1), :]
        gt[t] = jnp.broadcast_to(row, (128, 128)).T

    def bias_column():
        parts = [jnp.broadcast_to(bias_ref[k:k + 1, :], (128, 128)).T for k in range(3)]
        return jnp.concatenate(parts, axis=0)

    def hidden(cc):
        def stat(j, carry):
            s, q = carry
            v = xt[j].reshape(HALF, TOK).astype(F32)
            return s + jnp.sum(v, axis=0, keepdims=True), q + jnp.sum(v * v, axis=0, keepdims=True)

        zero = jnp.zeros((1, TOK), F32)
        s, q = lax.fori_loop(0, NZ, stat, (zero, zero))
        mean = s / WIDTH
        var = jnp.maximum(q / WIDTH - mean * mean, 0.0)
        inv = lax.rsqrt(var + floor_value)

        def norm(j, _):
            v = xt[pl.ds(2 * j, 2)].reshape(BLK, TOK).astype(F32)
            g = gt[pl.ds(3 * j, 3)].reshape(BLK, TOK)
            nx[j] = ((v - mean) * inv * g).astype(BF16)
            return 0

        lax.fori_loop(0, NR, norm, 0)
        return None

    def project(cc):
        def step(j, acc):
            w = w1[cc, pl.ds(2 * j, 2)].reshape(BLK, BLK)
            return acc + jnp.dot(w, nx[j], preferred_element_type=F32)

        acc = lax.fori_loop(0, NR, step, jnp.zeros((BLK, TOK), F32))
        hid[cc] = gelu(acc + bias_column()).astype(BF16)

    @pl.when(c == 0)
    def _():
        weights = (w1, w2)

        def full(w, cc, b):
            return weights[w].at[cc, pl.ds(2 * b, 2)]

        def half(w, cc, b, h):
            return weights[w].at[cc, 2 * b + h]

        def axis(cc):
            if cc == 0:
                return x, y, (lambda p, q: q * NP + p), (lambda p, q: dev(q, p, z, c))
            return y, x, (lambda p, q: p * NP + q), (lambda p, q: dev(p, q, z, c))

        def send(w, cc, ref, idx, to):
            remote(ref, ref, pl_send.at[w, cc], pl_recv.at[w, cc, idx], to).start()

        def arrived(w, cc, ref, idx):
            remote(ref, ref, pl_send.at[w, cc], pl_recv.at[w, cc, idx], partner).wait_recv()

        def push(w, cc, b):
            if w == 0 and cc == 0:
                return
            ref = full(w, cc, b)
            remote(ref, ref, wp_send.at[w, cc], wp_recv.at[w, cc, b], partner).start()

        def mod(v):
            return (v + NP) % NP

        offs = (0, -1, 1, 2)

        def own_sends(w, pred):
            @pl.when(pred(r))
            def _():
                for cc in (0, 1):
                    p, q, ident, at = axis(cc)
                    send(w, cc, full(w, cc, r), 0, at(mod(p + 1), q))
                    send(w, cc, full(w, cc, r), 1, at(mod(p - 1), q))
                for cc in (0, 1):
                    p, q, ident, at = axis(cc)
                    send(w, cc, full(w, cc, r), 4, at(p, mod(q + 1)))
                    send(w, cc, full(w, cc, r), 5, at(p, mod(q - 1)))
                if w == 1:
                    push(w, 0, r)

        def q_sends(w, cc, i, b):
            p, q, ident, at = axis(cc)
            send(w, cc, full(w, cc, b), 4 + 4 * i, at(p, mod(q + 1)))
            send(w, cc, full(w, cc, b), 5 + 4 * i, at(p, mod(q - 1)))

        def first_full(w, pred):
            for d in (0, 1):
                for cc in (0, 1):
                    p, q, ident, at = axis(cc)
                    b = ident(mod(p - 1), q) if d == 0 else ident(mod(p + 1), q)

                    @pl.when(pred(b))
                    def _():
                        arrived(w, cc, full(w, cc, b), d)
                        to = at(mod(p + 1), q) if d == 0 else at(mod(p - 1), q)
                        send(w, cc, half(w, cc, b, d), 2 + d, to)
                        q_sends(w, cc, 1 + d, b)
                        push(w, cc, b)

        def first_half(w, pred):
            for cc in (0, 1):
                p, q, ident, at = axis(cc)
                b = ident(mod(p + 2), q)

                @pl.when(pred(b))
                def _():
                    arrived(w, cc, half(w, cc, b, 0), 2)
                    arrived(w, cc, half(w, cc, b, 1), 3)
                    q_sends(w, cc, 3, b)
                    push(w, cc, b)

        def second_full(w, pred, i):
            for d in (0, 1):
                for cc in (0, 1):
                    p, q, ident, at = axis(cc)
                    b = ident(mod(p + offs[i]), mod(q - 1) if d == 0 else mod(q + 1))

                    @pl.when(pred(b))
                    def _():
                        arrived(w, cc, full(w, cc, b), 4 + 4 * i + d)
                        to = at(p, mod(q + 1)) if d == 0 else at(p, mod(q - 1))
                        send(w, cc, half(w, cc, b, d), 6 + 4 * i + d, to)
                        push(w, cc, b)

        def second_half(w, pred, i):
            for cc in (0, 1):
                p, q, ident, at = axis(cc)
                b = ident(mod(p + offs[i]), mod(q + 2))

                @pl.when(pred(b))
                def _():
                    arrived(w, cc, half(w, cc, b, 0), 6 + 4 * i)
                    arrived(w, cc, half(w, cc, b, 1), 7 + 4 * i)
                    push(w, cc, b)

        def events(w, pred):
            first_full(w, pred)
            second_full(w, pred, 0)
            first_half(w, pred)
            second_full(w, pred, 1)
            second_full(w, pred, 2)
            second_half(w, pred, 0)
            second_full(w, pred, 3)
            second_half(w, pred, 1)
            second_half(w, pred, 2)
            second_half(w, pred, 3)

        def every(b):
            return b >= 0

        def far(b):
            return (b - z // 2 - 4 + 2 * NR) % NR < NR // 2

        def near(b):
            return (b - z // 2 - 4 + 2 * NR) % NR >= NR // 2

        put_weight(win_ref, w1)
        wait_all(5)
        remote(xt.at[z, 0], xt.at[z, 0], own_send, own_recv, partner).start()
        remote(full(0, 1, r), full(0, 1, r), nb_send.at[0], nb_recv.at[0], partner).wait_recv()
        own_sends(0, every)
        put_weight(wout_ref, w2)
        lax.fori_loop(0, 48, lambda t, _: (spread_gain(t), 0)[1], 0)
        events(0, every)
        remote(full(1, 1, r), full(1, 1, r), nb_send.at[1], nb_recv.at[1], partner).wait_recv()
        own_sends(1, far)

        remote(xt.at[z, 1], xt.at[z, 1], own_send, own_recv, partner).wait_recv()

        def take(s, _):
            for h in (1, 0):
                a = (z + NZ - s) % NZ
                remote(xt.at[a, h], xt.at[a, h], push_send, ag_recv.at[0, s, h], partner).wait_recv()

                @pl.when(s < STEPS)
                def _():
                    b = (z + s) % NZ
                    remote(xt.at[b, h], xt.at[b, h], push_send, ag_recv.at[1, s, h], partner).wait_recv()

            return 0

        lax.fori_loop(1, STEPS + 1, take, 0)
        hidden(0)
        project(0)
        remote(hid.at[0], hid.at[0], hid_send, hid_recv, partner).start()
        events(1, far)
        own_sends(1, near)
        events(1, near)

        for w in (0, 1):
            for cc in (0, 1):
                ref = weights[w].at[cc, pl.ds(0, 30)]
                remote(ref, ref, pl_send.at[w, cc], pl_recv.at[w, cc, 0], partner).wait_send()
                if w == 1 and cc == 0:
                    ref = weights[w].at[cc, pl.ds(0, 32)]
                if w == 1 or cc == 1:
                    remote(ref, ref, wp_send.at[w, cc], wp_recv.at[w, cc, 0], partner).wait_send()
        remote(xt.at[z, 0], xt.at[z, 0], own_send, own_recv, partner).wait_send()
        remote(hid.at[0], hid.at[0], hid_send, hid_recv, partner).wait_send()
        remote(res.at[0], res.at[0], res_send, res_recv, partner).wait_recv()
        pad[0:FEAT, :] = res[0].astype(F32)

    @pl.when(c == 1)
    def _():
        wait_all(3)
        own1 = xt.at[z, 1]
        remote(own1, own1, ag_send, ag_recv.at[0, 1, 1], zup).start()
        remote(own1, own1, ag_send, ag_recv.at[1, 1, 1], zdn).start()
        remote(own1, own1, own_send, own_recv, partner).start()
        own0 = xt.at[z, 0]
        remote(own0, own0, own_send, own_recv, partner).wait_recv()
        remote(own0, own0, ag_send, ag_recv.at[0, 1, 0], zup).start()
        remote(own0, own0, ag_send, ag_recv.at[1, 1, 0], zdn).start()
        put_weight(win_ref, w1)
        wb = w1.at[1, pl.ds(2 * r, 2)]
        remote(wb, wb, nb_send.at[0], nb_recv.at[0], partner).start()

        def ring(s, _):
            for h in (1, 0):
                a = (z + NZ - s) % NZ
                ra = xt.at[a, h]
                remote(ra, ra, ag_send, ag_recv.at[0, s, h], zup).wait_recv()

                @pl.when(s < STEPS)
                def _():
                    remote(ra, ra, ag_send, ag_recv.at[0, s + 1, h], zup).start()

                remote(ra, ra, push_send, ag_recv.at[0, s, h], partner).start()

                @pl.when(s < STEPS)
                def _():
                    b = (z + s) % NZ
                    rb = xt.at[b, h]
                    remote(rb, rb, ag_send, ag_recv.at[1, s, h], zdn).wait_recv()

                    @pl.when(s < STEPS - 1)
                    def _():
                        remote(rb, rb, ag_send, ag_recv.at[1, s + 1, h], zdn).start()

                    remote(rb, rb, push_send, ag_recv.at[1, s, h], partner).start()

            for k in range(3):
                spread_gain(3 * (s - 1) + k)
            return 0

        ring(1, 0)
        put_weight(wout_ref, w2)
        wo = w2.at[1, pl.ds(2 * r, 2)]
        remote(wo, wo, nb_send.at[1], nb_recv.at[1], partner).start()
        lax.fori_loop(2, STEPS + 1, ring, 0)
        hidden(1)

        def take_weight(b, _):
            @pl.when(b != r)
            def _():
                ref = w1.at[1, pl.ds(2 * b, 2)]
                remote(ref, ref, wp_send.at[0, 1], wp_recv.at[0, 1, b], partner).wait_recv()

            return 0

        lax.fori_loop(0, NR, take_weight, 0)
        project(1)
        remote(hid.at[0], hid.at[0], hid_send, hid_recv, partner).wait_recv()

        def take_out(b):
            ra = w2.at[0, pl.ds(2 * b, 2)]
            remote(ra, ra, wp_send.at[1, 0], wp_recv.at[1, 0, b], partner).wait_recv()

            @pl.when(b != r)
            def _():
                rb = w2.at[1, pl.ds(2 * b, 2)]
                remote(rb, rb, wp_send.at[1, 1], wp_recv.at[1, 1, b], partner).wait_recv()

        def partial(d):
            return jnp.dot(w2[0, d], hid[0], preferred_element_type=F32) + jnp.dot(
                w2[1, d], hid[1], preferred_element_type=F32
            )

        def rs_copy(dr, s, h, to):
            return remote(
                rsout.at[dr, s, h], rsin.at[dr, s, h],
                rs_send.at[dr], rs_recv.at[dr, s, h], to,
            )

        def reduce(s, _):
            du = (z + STEPS - s) % NZ
            dd = (z + NZ - STEPS + 1 + s) % NZ

            @pl.when((s == 0) | (du % 2 == 1))
            def _():
                take_out(du // 2)

            part[0] = partial(du)

            @pl.when((s < STEPS - 1) & (dd % 2 == 0))
            def _():
                take_out(dd // 2)

            @pl.when(s < STEPS - 1)
            def _():
                part[1] = partial(dd)

            for h in (0, 1):
                rows = slice(FEAT * h, FEAT * h + FEAT)

                @pl.when(s > 0)
                def _():
                    rs_copy(0, s - 1, h, zup).wait_recv()
                    rsout[0, s, h] = (part[0, rows] + rsin[0, s - 1, h].astype(F32)).astype(BF16)

                @pl.when(s == 0)
                def _():
                    rsout[0, s, h] = part[0, rows].astype(BF16)

                rs_copy(0, s, h, zup).start()

                @pl.when((s > 0) & (s < STEPS - 1))
                def _():
                    rs_copy(1, s - 1, h, zdn).wait_recv()
                    rsout[1, s, h] = (part[1, rows] + rsin[1, s - 1, h].astype(F32)).astype(BF16)

                @pl.when(s == 0)
                def _():
                    rsout[1, s, h] = part[1, rows].astype(BF16)

                @pl.when(s < STEPS - 1)
                def _():
                    rs_copy(1, s, h, zdn).start()

            return 0

        lax.fori_loop(0, STEPS, reduce, 0)
        mine = partial(z)
        for h in (0, 1):
            rs_copy(0, STEPS - 1, h, zup).wait_recv()
            rs_copy(1, STEPS - 2, h, zdn).wait_recv()
            total = (
                xt[z, h].astype(F32)
                + mine[FEAT * h:FEAT * h + FEAT]
                + rsin[0, STEPS - 1, h].astype(F32)
                + rsin[1, STEPS - 2, h].astype(F32)
            )
            if h == 0:
                res[0] = total.astype(BF16)
                remote(res.at[0], res.at[0], res_send, res_recv, partner).start()
            else:
                pad[0:FEAT, :] = total

        remote(xt.at[pl.ds(0, NZ - 1)], xt.at[pl.ds(0, NZ - 1)], ag_send, own_recv, partner).wait_send()
        remote(xt.at[pl.ds(0, NZ - 1)], xt.at[pl.ds(0, NZ - 1)], push_send, own_recv, partner).wait_send()
        remote(own1, own1, own_send, own_recv, partner).wait_send()
        for w, ref in ((0, wb), (1, wo)):
            remote(ref, ref, nb_send.at[w], nb_recv.at[w], partner).wait_send()
        for dr, n in ((0, STEPS), (1, STEPS - 1)):
            ref = rsout.at[dr, pl.ds(0, n)]
            remote(ref, ref, rs_send.at[dr], own_recv, partner).wait_send()
        remote(res.at[0], res.at[0], res_send, res_recv, partner).wait_send()

    out_ref[...] = pad[...].T[:, 0:FEAT].astype(BF16)


def body(tokens, norm_gain, hidden_bias, weight_in, weight_out):
    dma = pltpu.SemaphoreType.DMA
    vmem = pl.BlockSpec(memory_space=pltpu.VMEM)
    return pl.pallas_call(
        kernel,
        out_shape=jax.ShapeDtypeStruct((TOK, FEAT), BF16),
        in_specs=[vmem] * 5,
        out_specs=vmem,
        scratch_shapes=[
            pltpu.VMEM((NZ, 2, FEAT, TOK), BF16),
            pltpu.VMEM((NR, BLK, TOK), BF16),
            pltpu.VMEM((2, NZ, HALF, BLK), BF16),
            pltpu.VMEM((2, NZ, HALF, BLK), BF16),
            pltpu.VMEM((48, 128, 128), F32),
            pltpu.VMEM((2, BLK, TOK), BF16),
            pltpu.VMEM((128, 128), F32),
            pltpu.VMEM((2, STEPS, 2, FEAT, TOK), BF16),
            pltpu.VMEM((2, STEPS, 2, FEAT, TOK), BF16),
            pltpu.VMEM((1, FEAT, TOK), BF16),
            pltpu.VMEM((2, HALF, TOK), F32),
            dma, dma((2, STEPS + 1, 2)), dma, dma, dma,
            dma((2, 2)), dma((2, 2, 20)), dma((2, 2)), dma((2, 2, NR)), dma((2,)), dma((2,)),
            dma, dma, dma((2,)), dma((2, STEPS, 2)), dma, dma,
        ],
        compiler_params=pltpu.CompilerParams(
            collective_id=0, has_side_effects=True, vmem_limit_bytes=60 * 1024 * 1024
        ),
    )(
        tokens,
        norm_gain.reshape(48, 128),
        hidden_bias.reshape(3, 128),
        weight_in,
        weight_out,
    )


def solution(mesh):
    finer = Mesh(mesh.devices.reshape(4, 4, 32, 2), ("rows_0", "rows_1", "mp_0", "mp_1"))
    placed = (P(ROWS, MP), P(), P(MP), P(ROWS, MP), P(MP, ROWS))
    return jax.shard_map(body, mesh=finer, in_specs=placed, out_specs=P(ROWS, MP), check_vma=False)
```

```python
import jax
import jax.numpy as jnp
from jax import lax
from jax.experimental import pallas as pl
from jax.experimental.pallas import tpu as pltpu
from jax.sharding import Mesh
from jax.sharding import PartitionSpec as P

MP = ("mp_0", "mp_1")
ROWS = ("rows_0", "rows_1")
NZ = 32
NP = 4
NR = 16
TOK = 128
FEAT = 96
BLK = 384
HALF = 192
WIDTH = NZ * 2 * FEAT
STEPS = NZ // 2
PAIRS = STEPS // 2
F32 = jnp.float32
BF16 = jnp.bfloat16

floor_value = 0.1


def gelu(v):
    return 0.5 * v * (1.0 + lax.erf(v * 0.7071067811865476))


def kernel(
    tok_ref, gain_ref, bias_ref, win_ref, wout_ref, out_ref,
    xt, x4, nx, w1, w2, gt, st, sums, pout, pin, hid, cin, cout, lin, lout, res, part, acc,
    ag_send, ag_recv, y_send, x_send, x_recv, st_send, st_recv, p_send, p_recv, own_send, own_recv,
    pl_send, pl_recv, wp_send, wp_recv, nb_send, nb_recv,
    hid_send, hid_recv, c_send, c_recv, l_send, l_recv, res_send, res_recv,
):
    y = lax.axis_index("rows_0")
    x = lax.axis_index("rows_1")
    z = lax.axis_index("mp_0")
    c = lax.axis_index("mp_1")
    r = y * NP + x

    def dev(yy, xx, zz, cc):
        return (yy, xx, zz, cc)

    partner = dev(y, x, z, 1 - c)
    zup = dev(y, x, (z + 1) % NZ, c)
    zdn = dev(y, x, (z + NZ - 1) % NZ, c)
    zup2 = dev(y, x, (z + 2) % NZ, c)
    zdn2 = dev(y, x, (z + NZ - 2) % NZ, c)

    def remote(src, dst, ssem, rsem, to):
        return pltpu.make_async_remote_copy(
            src_ref=src, dst_ref=dst, send_sem=ssem, recv_sem=rsem,
            device_id=to, device_id_type=pl.DeviceIdType.MESH,
        )

    def signal_all(targets):
        bar = pltpu.get_barrier_semaphore()
        for t in targets:
            pl.semaphore_signal(bar, inc=1, device_id=t, device_id_type=pl.DeviceIdType.MESH)

    def wait_all(n):
        pl.semaphore_wait(pltpu.get_barrier_semaphore(), n)

    def peer(k, cc):
        return dev((y + k) % NP, x, z, cc)

    peers = [peer(k, cc) for k in (1, 2, 3) for cc in (0, 1)]

    @pl.when(c == 0)
    def _():
        signal_all([partner, dev(y, (x + 1) % NP, z, c), dev(y, (x + NP - 1) % NP, z, c)] + peers)

    @pl.when(c == 1)
    def _():
        signal_all([partner, zup, zdn, zup2, zdn2] + peers)


    def put_weight(src, dst):
        t = src[...].astype(F32).T.astype(BF16)
        dst[c, 2 * r] = t[0:HALF, :]
        dst[c, 2 * r + 1] = t[HALF:BLK, :]

    def spread_gain(t):
        row = gain_ref[pl.ds(12 * y + t, 1), :]
        gt[t] = jnp.broadcast_to(row, (128, 128)).T

    def bias_column():
        parts = [jnp.broadcast_to(bias_ref[k:k + 1, :], (128, 128)).T for k in range(3)]
        return jnp.concatenate(parts, axis=0)

    def get_stats(k):
        b = (y + k) % NP
        remote(st.at[b], st.at[b], st_send.at[0], st_recv.at[b], partner).wait_recv()

    def project(cc, ks):
        w = [w1[cc, pl.ds(2 * (NP * y + j), 2)].reshape(BLK, BLK) for j in range(NP)]
        for n, k in enumerate(ks):
            b = (y + k) % NP
            mean = st[b, 0, 0:1, :]
            inv = st[b, 1, 0:1, :]

            def norm(j, _):
                v = x4[b, pl.ds(2 * j, 2)].reshape(BLK, TOK).astype(F32)
                g = gt[pl.ds(3 * j, 3)].reshape(BLK, TOK)
                nx[j, :, TOK * n:TOK * n + TOK] = ((v - mean) * inv * g).astype(BF16)
                return 0

            lax.fori_loop(0, NP, norm, 0)
        total = jnp.dot(w[0], nx[0], preferred_element_type=F32)
        for j in range(1, NP):
            total = total + jnp.dot(w[j], nx[j], preferred_element_type=F32)
        return total

    def shares(cc):
        def give(k, v):
            b = (y + k) % NP
            pout[b] = v.astype(BF16)
            remote(pout.at[b], pin.at[y], p_send, p_recv.at[y], dev(b, x, z, cc)).start()

        v = project(cc, (2, 1))
        give(2, v[:, 0:TOK])
        give(1, v[:, TOK:])
        v = project(cc, (3, 0))
        give(3, v[:, 0:TOK])
        acc[...] = v[:, TOK:] + bias_column()

    def activate(cc):
        v = acc[...]
        for k in (1, 2, 3):
            b = (y + k) % NP
            remote(pout.at[b], pin.at[b], p_send, p_recv.at[b], partner).wait_recv()
            v = v + pin[b].astype(F32)
        hid[cc] = gelu(v).astype(BF16)

    @pl.when(c == 0)
    def _():
        weights = (w1, w2)

        def full(w, cc, b):
            return weights[w].at[cc, pl.ds(2 * b, 2)]

        def half(w, cc, b, h):
            return weights[w].at[cc, 2 * b + h]

        def axis(cc):
            if cc == 0:
                return x, y, (lambda p, q: q * NP + p), (lambda p, q: dev(q, p, z, c))
            return y, x, (lambda p, q: p * NP + q), (lambda p, q: dev(p, q, z, c))

        def send(w, cc, ref, idx, to):
            remote(ref, ref, pl_send.at[w, cc], pl_recv.at[w, cc, idx], to).start()

        def arrived(w, cc, ref, idx):
            remote(ref, ref, pl_send.at[w, cc], pl_recv.at[w, cc, idx], partner).wait_recv()

        def push(w, cc, b):
            ref = full(w, cc, b)
            remote(ref, ref, wp_send.at[w, cc], wp_recv.at[w, cc, b], partner).start()

        def mod(v):
            return (v + NP) % NP

        offs = (0, -1, 1, 2)

        def row_block(k):
            return NP * y + (x + k + NP) % NP

        def row_dev(k):
            return dev(y, (x + k + NP) % NP, z, c)

        def row_own():
            for cc in (0, 1):
                send(0, cc, full(0, cc, r), 0, row_dev(1))
                send(0, cc, full(0, cc, r), 1, row_dev(-1))

        def row_full():
            for cc in (0, 1):
                for d, k in ((0, -1), (1, 1)):
                    b = row_block(k)
                    arrived(0, cc, full(0, cc, b), d)
                    send(0, cc, half(0, cc, b, d), 2 + d, row_dev(-k))
                    if cc == 1:
                        push(0, cc, b)

        def row_half():
            for cc in (0, 1):
                b = row_block(2)
                arrived(0, cc, half(0, cc, b, 0), 2)
                arrived(0, cc, half(0, cc, b, 1), 3)
                if cc == 1:
                    push(0, cc, b)

        def own_sends():
            for cc in (1, 0):
                p, q, ident, at = axis(cc)
                send(1, cc, full(1, cc, r), 0, at(mod(p + 1), q))
                send(1, cc, full(1, cc, r), 1, at(mod(p - 1), q))
            for cc in (0, 1):
                q_sends(cc, 0, r)
            push(1, 0, r)

        def q_sends(cc, i, b):
            p, q, ident, at = axis(cc)
            send(1, cc, full(1, cc, b), 4 + 4 * i, at(p, mod(q + 1)))
            send(1, cc, full(1, cc, b), 5 + 4 * i, at(p, mod(q - 1)))

        def first_full(cc):
            for d, k in ((0, -1), (1, 1)):
                p, q, ident, at = axis(cc)
                b = ident(mod(p + k), q)
                arrived(1, cc, full(1, cc, b), d)
                send(1, cc, half(1, cc, b, d), 2 + d, at(mod(p - k), q))
                q_sends(cc, 1 + d, b)
                push(1, cc, b)

        def first_half(cc):
            p, q, ident, at = axis(cc)
            b = ident(mod(p + 2), q)
            arrived(1, cc, half(1, cc, b, 0), 2)
            arrived(1, cc, half(1, cc, b, 1), 3)
            q_sends(cc, 3, b)
            push(1, cc, b)

        def second_full(cc, i):
            for d, k in ((0, -1), (1, 1)):
                p, q, ident, at = axis(cc)
                b = ident(mod(p + offs[i]), mod(q + k))
                arrived(1, cc, full(1, cc, b), 4 + 4 * i + d)
                send(1, cc, half(1, cc, b, d), 6 + 4 * i + d, at(p, mod(q - k)))
                push(1, cc, b)

        def second_half(cc, i):
            p, q, ident, at = axis(cc)
            b = ident(mod(p + offs[i]), mod(q + 2))
            arrived(1, cc, half(1, cc, b, 0), 6 + 4 * i)
            arrived(1, cc, half(1, cc, b, 1), 7 + 4 * i)
            push(1, cc, b)

        wait_all(9)
        remote(tok_ref, xt.at[z, 0], own_send, own_recv, partner).start()
        put_weight(win_ref, w1)
        remote(full(0, 1, r), full(0, 1, r), nb_send.at[0], nb_recv.at[0], partner).wait_recv()
        row_own()
        put_weight(wout_ref, w2)
        remote(full(1, 1, r), full(1, 1, r), nb_send.at[1], nb_recv.at[1], partner).wait_recv()
        own_sends()
        lax.fori_loop(0, 12, lambda t, _: (spread_gain(t), 0)[1], 0)
        first_full(1)
        second_full(0, 0)
        row_full()
        first_half(1)
        first_full(0)
        second_full(1, 0)
        row_half()
        first_half(0)
        for i in (1, 2):
            second_full(0, i)
            second_full(1, i)
        second_half(0, 0)
        second_half(1, 0)
        second_full(0, 3)
        second_full(1, 3)

        def take(j, _):
            for b in range(NP):
                for h in (0, 1):
                    ref = x4.at[b, j, h]
                    remote(ref, ref, x_send, x_recv.at[b, j, h], partner).wait_recv()
            return 0

        lax.fori_loop(0, 8, take, 0)
        for k in range(NP):
            get_stats(k)
        shares(0)
        for i in (1, 2, 3):
            second_half(0, i)
            second_half(1, i)
        activate(0)
        remote(hid.at[0], hid.at[0], hid_send, hid_recv, partner).start()

        for cc in (0, 1):
            ref = w1.at[cc, pl.ds(0, 6)]
            remote(ref, ref, pl_send.at[0, cc], pl_recv.at[0, cc, 0], partner).wait_send()
            ref = w2.at[cc, pl.ds(0, 30)]
            remote(ref, ref, pl_send.at[1, cc], pl_recv.at[1, cc, 0], partner).wait_send()
            ref = w2.at[cc, pl.ds(0, 32 - 2 * cc)]
            remote(ref, ref, wp_send.at[1, cc], wp_recv.at[1, cc, 0], partner).wait_send()
        ref = w1.at[1, pl.ds(0, 6)]
        remote(ref, ref, wp_send.at[0, 1], wp_recv.at[0, 1, 0], partner).wait_send()
        remote(pout.at[pl.ds(0, 3)], pout.at[pl.ds(0, 3)], p_send, own_recv, partner).wait_send()
        remote(tok_ref, xt.at[z, 0], own_send, own_recv, partner).wait_send()
        remote(hid.at[0], hid.at[0], hid_send, hid_recv, partner).wait_send()
        remote(res.at[0], res.at[0], res_send, res_recv, partner).wait_recv()
        out_ref[...] = res[0]

    @pl.when(c == 1)
    def _():
        own1 = xt.at[z, 1]
        own0 = xt.at[z, 0]
        xt[z, 1] = tok_ref[...]
        sums[...] = jnp.zeros((2, 8, TOK), F32)
        wait_all(11)

        def pass_on(src, a, h, dr, s):
            ref = xt.at[a, h]
            remote(src, ref, ag_send, ag_recv.at[dr, s + 2, h], (zup2, zdn2)[dr]).start()
            remote(src, ref, ag_send, ag_recv.at[dr, s + 1, h], (zup, zdn)[dr]).start()

        pass_on(tok_ref, z, 1, 0, 0)
        pass_on(tok_ref, z, 1, 1, 0)

        def deliver(a, h):
            g = a // 8
            k = a % 8

            @pl.when(g != y)
            def _():
                remote(xt.at[a, h], x4.at[y, k, h], y_send, x_recv.at[y, k, h], dev(g, x, z, 1)).start()

            @pl.when(g == y)
            def _():
                remote(xt.at[a, h], x4.at[y, k, h], x_send, x_recv.at[y, k, h], partner).start()
                x4[y, k, h] = xt[a, h]

            v = xt[a, h].astype(F32).reshape(FEAT // 8, 8, TOK)
            sums[0] = sums[0] + jnp.sum(v, axis=0)
            sums[1] = sums[1] + jnp.sum(v * v, axis=0)

        def relay(a):
            @pl.when(a // 8 == y)
            def _():
                for k in (1, 2, 3):
                    b = (y + k) % NP
                    for h in (1, 0):
                        ref = x4.at[b, a % 8, h]
                        remote(ref, ref, x_send, x_recv.at[b, a % 8, h], partner).wait_recv()
                        remote(ref, ref, x_send, x_recv.at[b, a % 8, h], partner).start()

        put_weight(win_ref, w1)
        wb = w1.at[1, pl.ds(2 * r, 2)]
        remote(wb, wb, nb_send.at[0], nb_recv.at[0], partner).start()
        deliver(z, 1)
        remote(own0, own0, own_send, own_recv, partner).wait_recv()
        pass_on(own0, z, 0, 0, 0)
        pass_on(own0, z, 0, 1, 0)
        put_weight(wout_ref, w2)
        wo = w2.at[1, pl.ds(2 * r, 2)]
        remote(wo, wo, nb_send.at[1], nb_recv.at[1], partner).start()
        deliver(z, 0)

        def came(dr, a, s, h):
            ref = xt.at[a, h]
            remote(ref, ref, ag_send, ag_recv.at[dr, s, h], zup).wait_recv()

        def relays(i):
            relay((z + NZ - 2 * i) % NZ)
            relay((z + NZ - 2 * i + 1) % NZ)
            relay((z + 2 * i - 1) % NZ)

            @pl.when(i < PAIRS)
            def _():
                relay((z + 2 * i) % NZ)

        def ring(i, _):
            a = (z + NZ - 2 * i) % NZ
            b = (z + 2 * i) % NZ
            a1 = (z + NZ - 2 * i + 1) % NZ
            b1 = (z + 2 * i - 1) % NZ
            for h in (1, 0):
                came(0, a, 2 * i, h)

                @pl.when(i < PAIRS)
                def _():
                    pass_on(xt.at[a, h], a, h, 0, 2 * i)
                    came(1, b, 2 * i, h)

                    @pl.when(i < PAIRS - 1)
                    def _():
                        remote(xt.at[b, h], xt.at[b, h], ag_send, ag_recv.at[1, 2 * i + 2, h], zdn2).start()

                    remote(xt.at[b, h], xt.at[b, h], ag_send, ag_recv.at[1, 2 * i + 1, h], zdn).start()

            for h in (1, 0):
                came(0, a1, 2 * i - 1, h)
                deliver(a1, h)
                came(1, b1, 2 * i - 1, h)
                deliver(b1, h)
                deliver(a, h)

                @pl.when(i < PAIRS)
                def _():
                    deliver(b, h)

            @pl.when(i == 2)
            def _():
                relay(z)

            @pl.when(i > 2)
            def _():
                relays(i - 2)

            @pl.when(i <= 6)
            def _():
                spread_gain(2 * i - 2)
                spread_gain(2 * i - 1)

            return 0

        lax.fori_loop(1, PAIRS + 1, ring, 0)
        mean = jnp.sum(sums[0], axis=0, keepdims=True) / WIDTH
        var = jnp.maximum(jnp.sum(sums[1], axis=0, keepdims=True) / WIDTH - mean * mean, 0.0)
        st[y, 0] = jnp.broadcast_to(mean, (8, TOK))
        st[y, 1] = jnp.broadcast_to(lax.rsqrt(var + floor_value), (8, TOK))
        for n, to in enumerate(peers + [partner]):
            remote(st.at[y], st.at[y], st_send.at[n], st_recv.at[y], to).start()
        relays(PAIRS - 1)
        relays(PAIRS)

        def take_weight(k, _):
            b = NP * y + (x + k) % NP
            ref = w1.at[1, pl.ds(2 * b, 2)]
            remote(ref, ref, wp_send.at[0, 1], wp_recv.at[0, 1, b], partner).wait_recv()
            return 0

        lax.fori_loop(1, NP, take_weight, 0)
        for k in (1, 2, 3):
            get_stats(k)
        shares(1)
        activate(1)
        remote(hid.at[0], hid.at[0], hid_send, hid_recv, partner).wait_recv()

        def take_out(b):
            ra = w2.at[0, pl.ds(2 * b, 2)]
            remote(ra, ra, wp_send.at[1, 0], wp_recv.at[1, 0, b], partner).wait_recv()

            @pl.when(b != r)
            def _():
                rb = w2.at[1, pl.ds(2 * b, 2)]
                remote(rb, rb, wp_send.at[1, 1], wp_recv.at[1, 1, b], partner).wait_recv()

        def partial(d):
            return jnp.dot(w2[0, d], hid[0], preferred_element_type=F32) + jnp.dot(
                w2[1, d], hid[1], preferred_element_type=F32
            )

        def chain(dr, i, h):
            return remote(
                cout.at[dr, i, h], cin.at[dr, i, h], c_send.at[dr], c_recv.at[dr, i, h], (zup2, zdn2)[dr]
            )

        def link(dr, i):
            return remote(
                lout.at[dr, i], lin.at[dr, i], l_send.at[dr], l_recv.at[dr, i], (zup, zdn)[dr]
            )

        def lend(dr, i, d):
            v = partial(d).astype(BF16)
            lout[dr, i, 0] = v[0:FEAT]
            lout[dr, i, 1] = v[FEAT:HALF]
            link(dr, i).start()

        def carry(dr, i, h, terms):
            v = part[dr, FEAT * h:FEAT * h + FEAT]
            for t in terms:
                v = v + t.astype(F32)
            cout[dr, i, h] = v.astype(BF16)
            chain(dr, i, h).start()

        lax.fori_loop(0, NR, lambda b, _: (take_out(b), 0)[1], 0)
        part[0] = partial((z + STEPS) % NZ)
        carry(0, 0, 0, ())
        carry(0, 0, 1, ())
        lend(1, 0, (z + NZ - STEPS + 1) % NZ)
        lend(0, 0, (z + STEPS - 1) % NZ)
        part[1] = partial((z + NZ - STEPS + 2) % NZ)
        link(1, 0).wait_recv()
        carry(1, 0, 0, (lin[1, 0, 0],))
        carry(1, 0, 1, (lin[1, 0, 1],))

        def reduce(i, _):
            lend(1, i, (z + NZ - STEPS + 1 + 2 * i) % NZ)
            lend(0, i, (z + STEPS - 1 - 2 * i) % NZ)
            part[0] = partial((z + STEPS - 2 * i) % NZ)

            @pl.when(i < PAIRS - 1)
            def _():
                part[1] = partial((z + NZ - STEPS + 2 + 2 * i) % NZ)

            link(0, i - 1).wait_recv()
            link(1, i).wait_recv()
            for h in (0, 1):
                chain(0, i - 1, h).wait_recv()
                carry(0, i, h, (cin[0, i - 1, h], lin[0, i - 1, h]))

                @pl.when(i < PAIRS - 1)
                def _():
                    chain(1, i - 1, h).wait_recv()
                    carry(1, i, h, (cin[1, i - 1, h], lin[1, i, h]))

            return 0

        lax.fori_loop(1, PAIRS, reduce, 0)
        mine = partial(z)
        link(0, PAIRS - 1).wait_recv()
        for h in (0, 1):
            chain(0, PAIRS - 1, h).wait_recv()
            chain(1, PAIRS - 2, h).wait_recv()
            total = (
                xt[z, h].astype(F32)
                + mine[FEAT * h:FEAT * h + FEAT]
                + (cin[0, PAIRS - 1, h].astype(F32) + lin[0, PAIRS - 1, h].astype(F32))
                + (cin[1, PAIRS - 2, h].astype(F32) + lin[1, PAIRS - 1, h].astype(F32))
            )
            if h == 0:
                res[0] = total.astype(BF16)
                remote(res.at[0], res.at[0], res_send, res_recv, partner).start()
            else:
                out_ref[...] = total.astype(BF16)

        remote(xt.at[pl.ds(0, NZ - 1)], xt.at[pl.ds(0, NZ - 1)], ag_send, own_recv, partner).wait_send()
        remote(xt.at[pl.ds(0, 24)], xt.at[pl.ds(0, 24)], y_send, own_recv, partner).wait_send()
        remote(x4, x4, x_send, own_recv, partner).wait_send()
        for n in range(7):
            remote(st.at[y], st.at[y], st_send.at[n], own_recv, partner).wait_send()
        remote(pout.at[pl.ds(0, 3)], pout.at[pl.ds(0, 3)], p_send, own_recv, partner).wait_send()
        for w, ref in ((0, wb), (1, wo)):
            remote(ref, ref, nb_send.at[w], nb_recv.at[w], partner).wait_send()
        for dr, n in ((0, PAIRS), (1, PAIRS - 1)):
            ref = cout.at[dr, pl.ds(0, n)]
            remote(ref, ref, c_send.at[dr], own_recv, partner).wait_send()
            ref = lout.at[dr]
            remote(ref, ref, l_send.at[dr], own_recv, partner).wait_send()
        remote(res.at[0], res.at[0], res_send, res_recv, partner).wait_send()


def body(tokens, norm_gain, hidden_bias, weight_in, weight_out):
    dma = pltpu.SemaphoreType.DMA
    vmem = pl.BlockSpec(memory_space=pltpu.VMEM)
    return pl.pallas_call(
        kernel,
        out_shape=jax.ShapeDtypeStruct((FEAT, TOK), BF16),
        in_specs=[vmem] * 5,
        out_specs=vmem,
        scratch_shapes=[
            pltpu.VMEM((NZ, 2, FEAT, TOK), BF16),
            pltpu.VMEM((NP, 8, 2, FEAT, TOK), BF16),
            pltpu.VMEM((NP, BLK, 2 * TOK), BF16),
            pltpu.VMEM((2, NZ, HALF, BLK), BF16),
            pltpu.VMEM((2, NZ, HALF, BLK), BF16),
            pltpu.VMEM((12, 128, 128), F32),
            pltpu.VMEM((NP, 2, 8, TOK), F32),
            pltpu.VMEM((2, 8, TOK), F32),
            pltpu.VMEM((NP, BLK, TOK), BF16),
            pltpu.VMEM((NP, BLK, TOK), BF16),
            pltpu.VMEM((2, BLK, TOK), BF16),
            pltpu.VMEM((2, PAIRS, 2, FEAT, TOK), BF16),
            pltpu.VMEM((2, PAIRS, 2, FEAT, TOK), BF16),
            pltpu.VMEM((2, PAIRS, 2, FEAT, TOK), BF16),
            pltpu.VMEM((2, PAIRS, 2, FEAT, TOK), BF16),
            pltpu.VMEM((1, FEAT, TOK), BF16),
            pltpu.VMEM((2, HALF, TOK), F32),
            pltpu.VMEM((BLK, TOK), F32),
            dma, dma((2, STEPS + 1, 2)), dma, dma, dma((NP, 8, 2)), dma((7,)), dma((NP,)),
            dma, dma((NP,)), dma, dma,
            dma((2, 2)), dma((2, 2, 20)), dma((2, 2)), dma((2, 2, NR)), dma((2,)), dma((2,)),
            dma, dma, dma((2,)), dma((2, PAIRS, 2)), dma((2,)), dma((2, PAIRS)), dma, dma,
        ],
        compiler_params=pltpu.CompilerParams(
            collective_id=0, has_side_effects=True, vmem_limit_bytes=60 * 1024 * 1024
        ),
    )(
        tokens.T,
        norm_gain.reshape(48, 128),
        hidden_bias.reshape(3, 128),
        weight_in,
        weight_out,
    ).T


def solution(mesh):
    finer = Mesh(mesh.devices.reshape(4, 4, 32, 2), ("rows_0", "rows_1", "mp_0", "mp_1"))
    placed = (P(ROWS, MP), P(), P(MP), P(ROWS, MP), P(MP, ROWS))
    return jax.shard_map(body, mesh=finer, in_specs=placed, out_specs=P(ROWS, MP), check_vma=False)
```

```python
import jax
import jax.numpy as jnp
from jax import lax
from jax.experimental import pallas as pl
from jax.experimental.pallas import tpu as pltpu
from jax.sharding import Mesh
from jax.sharding import PartitionSpec as P

MP = ("mp_0", "mp_1")
ROWS = ("rows_0", "rows_1")
NZ = 32
NP = 4
NR = 16
TOK = 128
FEAT = 96
BLK = 384
HALF = 192
WIDTH = NZ * 2 * FEAT
STEPS = NZ // 2
PAIRS = STEPS // 2
F32 = jnp.float32
BF16 = jnp.bfloat16

floor_value = 0.1


def gelu(v):
    return 0.5 * v * (1.0 + lax.erf(v * 0.7071067811865476))


def kernel(
    tok_ref, gain_ref, bias_ref, win_ref, wout_ref, out_ref,
    xt, x4, nx, w1, w2, gt, st, sums, pout, pin, hid, cin, cout, lin, lout, res, part, acc, pout0, pin0,
    ag_send, ag_recv, y_send, x_send, x_recv, st_send, st_recv, p_send, p_recv, own_send, own_recv,
    pl_send, pl_recv, wp_send, wp_recv, nb_send, nb_recv,
    hid_send, hid_recv, c_send, c_recv, l_send, l_recv, res_send, res_recv,
):
    y = lax.axis_index("rows_0")
    x = lax.axis_index("rows_1")
    z = lax.axis_index("mp_0")
    c = lax.axis_index("mp_1")
    r = y * NP + x

    def dev(yy, xx, zz, cc):
        return (yy, xx, zz, cc)

    partner = dev(y, x, z, 1 - c)
    zup = dev(y, x, (z + 1) % NZ, c)
    zdn = dev(y, x, (z + NZ - 1) % NZ, c)
    zup2 = dev(y, x, (z + 2) % NZ, c)
    zdn2 = dev(y, x, (z + NZ - 2) % NZ, c)

    def remote(src, dst, ssem, rsem, to):
        return pltpu.make_async_remote_copy(
            src_ref=src, dst_ref=dst, send_sem=ssem, recv_sem=rsem,
            device_id=to, device_id_type=pl.DeviceIdType.MESH,
        )

    def signal_all(targets):
        bar = pltpu.get_barrier_semaphore()
        for t in targets:
            pl.semaphore_signal(bar, inc=1, device_id=t, device_id_type=pl.DeviceIdType.MESH)

    def wait_all(n):
        pl.semaphore_wait(pltpu.get_barrier_semaphore(), n)

    def peer(k, cc):
        return dev((y + k) % NP, x, z, cc)

    peers = [peer(k, cc) for k in (1, 2, 3) for cc in (0, 1)]

    @pl.when(c == 0)
    def _():
        signal_all([partner, dev(y, (x + 1) % NP, z, c), dev(y, (x + NP - 1) % NP, z, c)] + peers)

    @pl.when(c == 1)
    def _():
        signal_all([partner, zup, zdn, zup2, zdn2] + peers)


    def put_weight(src, dst):
        t = src[...].astype(F32).T.astype(BF16)
        dst[c, 2 * r] = t[0:HALF, :]
        dst[c, 2 * r + 1] = t[HALF:BLK, :]

    def spread_gain(t):
        row = gain_ref[pl.ds(12 * y + t, 1), :]
        gt[t] = jnp.broadcast_to(row, (128, 128)).T

    def bias_column():
        parts = [jnp.broadcast_to(bias_ref[k:k + 1, :], (128, 128)).T for k in range(3)]
        return jnp.concatenate(parts, axis=0)

    def get_stats(k):
        b = (y + k) % NP
        remote(st.at[b], st.at[b], st_send.at[0], st_recv.at[b], partner).wait_recv()

    def project(cc, ks):
        w = [w1[cc, pl.ds(2 * (NP * y + j), 2)].reshape(BLK, BLK) for j in range(NP)]
        for n, k in enumerate(ks):
            b = (y + k) % NP
            mean = st[b, 0, 0:1, :]
            inv = st[b, 1, 0:1, :]

            def norm(j, _):
                v = x4[b, pl.ds(2 * j, 2)].reshape(BLK, TOK).astype(F32)
                g = gt[pl.ds(3 * j, 3)].reshape(BLK, TOK)
                nx[j, :, TOK * n:TOK * n + TOK] = ((v - mean) * inv * g).astype(BF16)
                return 0

            lax.fori_loop(0, NP, norm, 0)
        total = jnp.dot(w[0], nx[0], preferred_element_type=F32)
        for j in range(1, NP):
            total = total + jnp.dot(w[j], nx[j], preferred_element_type=F32)
        return total

    def give(cc, k, v):
        b = (y + k) % NP
        pout[b] = v.astype(BF16)
        remote(pout.at[b], pin.at[y], p_send, p_recv.at[y], dev(b, x, z, cc)).start()

    def first_shares(cc):
        v = project(cc, (2, 1))
        give(cc, 2, v[:, 0:TOK])
        give(cc, 1, v[:, TOK:])

    def last_shares(cc):
        v = project(cc, (3, 0))
        give(cc, 3, v[:, 0:TOK])
        acc[...] += v[:, TOK:]

    def activate(cc):
        v = acc[...]
        for k in (1, 2, 3):
            b = (y + k) % NP
            remote(pout.at[b], pin.at[b], p_send, p_recv.at[b], partner).wait_recv()
            v = v + pin[b].astype(F32)
        hid[cc] = gelu(v).astype(BF16)

    @pl.when(c == 0)
    def _():
        weights = (w1, w2)

        def full(w, cc, b):
            return weights[w].at[cc, pl.ds(2 * b, 2)]

        def half(w, cc, b, h):
            return weights[w].at[cc, 2 * b + h]

        def axis(cc):
            if cc == 0:
                return x, y, (lambda p, q: q * NP + p), (lambda p, q: dev(q, p, z, c))
            return y, x, (lambda p, q: p * NP + q), (lambda p, q: dev(p, q, z, c))

        def send(w, cc, ref, idx, to):
            remote(ref, ref, pl_send.at[w, cc], pl_recv.at[w, cc, idx], to).start()

        def arrived(w, cc, ref, idx):
            remote(ref, ref, pl_send.at[w, cc], pl_recv.at[w, cc, idx], partner).wait_recv()

        def push(w, cc, b):
            if cc == 0:
                return
            ref = full(w, cc, b)
            remote(ref, ref, wp_send.at[w, cc], wp_recv.at[w, cc, b], partner).start()

        def mod(v):
            return (v + NP) % NP

        offs = (0, -1, 1, 2)

        def row_block(k):
            return NP * y + (x + k + NP) % NP

        def row_dev(k):
            return dev(y, (x + k + NP) % NP, z, c)

        def row_own():
            for cc in (0, 1):
                send(0, cc, full(0, cc, r), 0, row_dev(1))
                send(0, cc, full(0, cc, r), 1, row_dev(-1))

        def row_full():
            for cc in (0, 1):
                for d, k in ((0, -1), (1, 1)):
                    b = row_block(k)
                    arrived(0, cc, full(0, cc, b), d)
                    send(0, cc, half(0, cc, b, d), 2 + d, row_dev(-k))
                    if cc == 1:
                        push(0, cc, b)

        def row_half():
            for cc in (0, 1):
                b = row_block(2)
                arrived(0, cc, half(0, cc, b, 0), 2)
                arrived(0, cc, half(0, cc, b, 1), 3)
                if cc == 1:
                    push(0, cc, b)

        def own_sends():
            for cc in (1, 0):
                p, q, ident, at = axis(cc)
                send(1, cc, full(1, cc, r), 0, at(mod(p + 1), q))
                send(1, cc, full(1, cc, r), 1, at(mod(p - 1), q))
            for cc in (0, 1):
                q_sends(cc, 0, r)

        def q_sends(cc, i, b):
            p, q, ident, at = axis(cc)
            send(1, cc, full(1, cc, b), 4 + 4 * i, at(p, mod(q + 1)))
            send(1, cc, full(1, cc, b), 5 + 4 * i, at(p, mod(q - 1)))

        def first_full(cc):
            for d, k in ((0, -1), (1, 1)):
                p, q, ident, at = axis(cc)
                b = ident(mod(p + k), q)
                arrived(1, cc, full(1, cc, b), d)
                send(1, cc, half(1, cc, b, d), 2 + d, at(mod(p - k), q))
                q_sends(cc, 1 + d, b)
                push(1, cc, b)

        def first_half(cc):
            p, q, ident, at = axis(cc)
            b = ident(mod(p + 2), q)
            arrived(1, cc, half(1, cc, b, 0), 2)
            arrived(1, cc, half(1, cc, b, 1), 3)
            q_sends(cc, 3, b)
            push(1, cc, b)

        def second_full(cc, i):
            for d, k in ((0, -1), (1, 1)):
                p, q, ident, at = axis(cc)
                b = ident(mod(p + offs[i]), mod(q + k))
                arrived(1, cc, full(1, cc, b), 4 + 4 * i + d)
                send(1, cc, half(1, cc, b, d), 6 + 4 * i + d, at(p, mod(q - k)))
                push(1, cc, b)

        def second_half(cc, i):
            p, q, ident, at = axis(cc)
            b = ident(mod(p + offs[i]), mod(q + 2))
            arrived(1, cc, half(1, cc, b, 0), 6 + 4 * i)
            arrived(1, cc, half(1, cc, b, 1), 7 + 4 * i)
            push(1, cc, b)

        wait_all(9)
        remote(tok_ref, xt.at[z, 0], own_send, own_recv, partner).start()
        put_weight(win_ref, w1)
        remote(full(0, 1, r), full(0, 1, r), nb_send.at[0], nb_recv.at[0], partner).wait_recv()
        row_own()
        put_weight(wout_ref, w2)
        remote(full(1, 1, r), full(1, 1, r), nb_send.at[1], nb_recv.at[1], partner).wait_recv()
        own_sends()
        lax.fori_loop(0, 12, lambda t, _: (spread_gain(t), 0)[1], 0)
        acc[...] = bias_column()
        first_full(1)
        second_full(0, 0)
        row_full()
        first_half(1)
        first_full(0)
        second_full(1, 0)
        row_half()
        first_half(0)
        for i in (1, 2):
            second_full(0, i)
            second_full(1, i)
        def take(j, _):
            for b in range(NP):
                for h in (0, 1):
                    ref = x4.at[b, j, h]
                    remote(ref, ref, x_send, x_recv.at[b, j, h], partner).wait_recv()
            return 0

        lax.fori_loop(0, 8, take, 0)
        for k in range(NP):
            get_stats(k)
        first_shares(0)
        last_shares(0)
        second_full(0, 3)
        second_full(1, 3)
        activate(0)
        for i in range(NP):
            second_half(0, i)
            second_half(1, i)

        def hand(d):
            d = (d + 2 * NZ) % NZ
            pout0[d] = jnp.dot(w2[0, d], hid[0], preferred_element_type=F32)
            remote(pout0.at[d], pin0.at[d], hid_send, hid_recv.at[d], partner).start()

        def hand_step(i, _):
            hand(z - STEPS + 1 + 2 * i)
            hand(z + STEPS - 1 - 2 * i)
            hand(z + STEPS - 2 * i)

            @pl.when(i < PAIRS - 1)
            def _():
                hand(z - STEPS + 2 + 2 * i)

            return 0

        hand(z + STEPS)
        hand(z - STEPS + 1)
        hand(z + STEPS - 1)
        hand(z - STEPS + 2)
        lax.fori_loop(1, PAIRS, hand_step, 0)
        hand(z)
        for cc in (0, 1):
            ref = w1.at[cc, pl.ds(0, 6)]
            remote(ref, ref, pl_send.at[0, cc], pl_recv.at[0, cc, 0], partner).wait_send()
            ref = w2.at[cc, pl.ds(0, 30)]
            remote(ref, ref, pl_send.at[1, cc], pl_recv.at[1, cc, 0], partner).wait_send()
        ref = w2.at[1, pl.ds(0, 30)]
        remote(ref, ref, wp_send.at[1, 1], wp_recv.at[1, 1, 0], partner).wait_send()
        ref = w1.at[1, pl.ds(0, 6)]
        remote(ref, ref, wp_send.at[0, 1], wp_recv.at[0, 1, 0], partner).wait_send()
        remote(pout.at[pl.ds(0, 3)], pout.at[pl.ds(0, 3)], p_send, own_recv, partner).wait_send()
        remote(tok_ref, xt.at[z, 0], own_send, own_recv, partner).wait_send()
        remote(pout0, pin0, hid_send, hid_recv.at[0], partner).wait_send()
        remote(res.at[0], res.at[0], res_send, res_recv, partner).wait_recv()
        out_ref[...] = res[0]

    @pl.when(c == 1)
    def _():
        acc[...] = bias_column()
        own1 = xt.at[z, 1]
        own0 = xt.at[z, 0]
        xt[z, 1] = tok_ref[...]
        sums[...] = jnp.zeros((2, 8, TOK), F32)
        wait_all(11)

        def pass_on(src, a, h, dr, s):
            ref = xt.at[a, h]
            remote(src, ref, ag_send, ag_recv.at[dr, s + 2, h], (zup2, zdn2)[dr]).start()
            remote(src, ref, ag_send, ag_recv.at[dr, s + 1, h], (zup, zdn)[dr]).start()

        pass_on(tok_ref, z, 1, 0, 0)
        pass_on(tok_ref, z, 1, 1, 0)

        def deliver(a, h):
            g = a // 8
            k = a % 8

            @pl.when(g != y)
            def _():
                remote(xt.at[a, h], x4.at[y, k, h], y_send, x_recv.at[y, k, h], dev(g, x, z, 1)).start()

            @pl.when(g == y)
            def _():
                remote(xt.at[a, h], x4.at[y, k, h], x_send, x_recv.at[y, k, h], partner).start()
                x4[y, k, h] = xt[a, h]

            v = xt[a, h].astype(F32).reshape(FEAT // 8, 8, TOK)
            sums[0] = sums[0] + jnp.sum(v, axis=0)
            sums[1] = sums[1] + jnp.sum(v * v, axis=0)

        def relay(a):
            @pl.when(a // 8 == y)
            def _():
                for k in (1, 2, 3):
                    b = (y + k) % NP
                    for h in (1, 0):
                        ref = x4.at[b, a % 8, h]
                        remote(ref, ref, x_send, x_recv.at[b, a % 8, h], partner).wait_recv()
                        remote(ref, ref, x_send, x_recv.at[b, a % 8, h], partner).start()

        put_weight(win_ref, w1)
        wb = w1.at[1, pl.ds(2 * r, 2)]
        remote(wb, wb, nb_send.at[0], nb_recv.at[0], partner).start()
        deliver(z, 1)
        remote(own0, own0, own_send, own_recv, partner).wait_recv()
        pass_on(own0, z, 0, 0, 0)
        pass_on(own0, z, 0, 1, 0)
        put_weight(wout_ref, w2)
        wo = w2.at[1, pl.ds(2 * r, 2)]
        remote(wo, wo, nb_send.at[1], nb_recv.at[1], partner).start()
        deliver(z, 0)

        def came(dr, a, s, h):
            ref = xt.at[a, h]
            remote(ref, ref, ag_send, ag_recv.at[dr, s, h], zup).wait_recv()

        def relays(i):
            relay((z + NZ - 2 * i) % NZ)
            relay((z + NZ - 2 * i + 1) % NZ)
            relay((z + 2 * i - 1) % NZ)

            @pl.when(i < PAIRS)
            def _():
                relay((z + 2 * i) % NZ)

        def ring(i, _):
            a = (z + NZ - 2 * i) % NZ
            b = (z + 2 * i) % NZ
            a1 = (z + NZ - 2 * i + 1) % NZ
            b1 = (z + 2 * i - 1) % NZ
            for h in (1, 0):
                came(0, a, 2 * i, h)

                @pl.when(i < PAIRS)
                def _():
                    pass_on(xt.at[a, h], a, h, 0, 2 * i)
                    came(1, b, 2 * i, h)

                    @pl.when(i < PAIRS - 1)
                    def _():
                        remote(xt.at[b, h], xt.at[b, h], ag_send, ag_recv.at[1, 2 * i + 2, h], zdn2).start()

                    remote(xt.at[b, h], xt.at[b, h], ag_send, ag_recv.at[1, 2 * i + 1, h], zdn).start()

            for h in (1, 0):
                came(0, a1, 2 * i - 1, h)
                deliver(a1, h)
                came(1, b1, 2 * i - 1, h)
                deliver(b1, h)
                deliver(a, h)

                @pl.when(i < PAIRS)
                def _():
                    deliver(b, h)

            @pl.when(i == 4)
            def _():
                relay(z)

            @pl.when(i > 4)
            def _():
                relays(i - 4)

            @pl.when(i <= 6)
            def _():
                spread_gain(2 * i - 2)
                spread_gain(2 * i - 1)

            return 0

        lax.fori_loop(1, PAIRS + 1, ring, 0)
        mean = jnp.sum(sums[0], axis=0, keepdims=True) / WIDTH
        var = jnp.maximum(jnp.sum(sums[1], axis=0, keepdims=True) / WIDTH - mean * mean, 0.0)
        st[y, 0] = jnp.broadcast_to(mean, (8, TOK))
        st[y, 1] = jnp.broadcast_to(lax.rsqrt(var + floor_value), (8, TOK))
        for n, to in enumerate(peers + [partner]):
            remote(st.at[y], st.at[y], st_send.at[n], st_recv.at[y], to).start()
        for i in range(PAIRS - 3, PAIRS + 1):
            relays(i)

        def take_weight(k, _):
            b = NP * y + (x + k) % NP
            ref = w1.at[1, pl.ds(2 * b, 2)]
            remote(ref, ref, wp_send.at[0, 1], wp_recv.at[0, 1, b], partner).wait_recv()
            return 0

        lax.fori_loop(1, NP, take_weight, 0)
        for k in (1, 2, 3):
            get_stats(k)
        first_shares(1)
        last_shares(1)
        activate(1)

        def take_out(b):
            @pl.when(b != r)
            def _():
                rb = w2.at[1, pl.ds(2 * b, 2)]
                remote(rb, rb, wp_send.at[1, 1], wp_recv.at[1, 1, b], partner).wait_recv()

        def partial(d):
            v = jnp.dot(w2[1, d], hid[1], preferred_element_type=F32)
            remote(pout0.at[d], pin0.at[d], hid_send, hid_recv.at[d], partner).wait_recv()
            return v + pin0[d]

        def chain(dr, i, h):
            return remote(
                cout.at[dr, i, h], cin.at[dr, i, h], c_send.at[dr], c_recv.at[dr, i, h], (zup2, zdn2)[dr]
            )

        def link(dr, i):
            return remote(
                lout.at[dr, i], lin.at[dr, i], l_send.at[dr], l_recv.at[dr, i], (zup, zdn)[dr]
            )

        def lend(dr, i, d):
            v = partial(d).astype(BF16)
            lout[dr, i, 0] = v[0:FEAT]
            lout[dr, i, 1] = v[FEAT:HALF]
            link(dr, i).start()

        def carry(dr, i, h, terms):
            v = part[dr, FEAT * h:FEAT * h + FEAT]
            for t in terms:
                v = v + t.astype(F32)
            cout[dr, i, h] = v.astype(BF16)
            chain(dr, i, h).start()

        def need(i):
            odd = z % 2

            @pl.when((i == 0) & (odd == 0))
            def _():
                take_out(((z + STEPS) % NZ) // 2)

            take_out(((z + STEPS - 1 + odd - 2 * i) % NZ) // 2)

            @pl.when((odd == 1) | (i < PAIRS - 1))
            def _():
                take_out(((z + NZ - STEPS + 2 - odd + 2 * i) % NZ) // 2)

        need(0)
        part[0] = partial((z + STEPS) % NZ)
        carry(0, 0, 0, ())
        carry(0, 0, 1, ())
        lend(1, 0, (z + NZ - STEPS + 1) % NZ)
        lend(0, 0, (z + STEPS - 1) % NZ)
        part[1] = partial((z + NZ - STEPS + 2) % NZ)
        link(1, 0).wait_recv()
        carry(1, 0, 0, (lin[1, 0, 0],))
        carry(1, 0, 1, (lin[1, 0, 1],))

        def reduce(i, _):
            need(i)
            lend(1, i, (z + NZ - STEPS + 1 + 2 * i) % NZ)
            lend(0, i, (z + STEPS - 1 - 2 * i) % NZ)
            part[0] = partial((z + STEPS - 2 * i) % NZ)

            @pl.when(i < PAIRS - 1)
            def _():
                part[1] = partial((z + NZ - STEPS + 2 + 2 * i) % NZ)

            link(0, i - 1).wait_recv()
            link(1, i).wait_recv()
            for h in (0, 1):
                chain(0, i - 1, h).wait_recv()
                carry(0, i, h, (cin[0, i - 1, h], lin[0, i - 1, h]))

                @pl.when(i < PAIRS - 1)
                def _():
                    chain(1, i - 1, h).wait_recv()
                    carry(1, i, h, (cin[1, i - 1, h], lin[1, i, h]))

            return 0

        lax.fori_loop(1, PAIRS, reduce, 0)
        mine = partial(z)
        link(0, PAIRS - 1).wait_recv()
        for h in (0, 1):
            chain(0, PAIRS - 1, h).wait_recv()
            chain(1, PAIRS - 2, h).wait_recv()
            total = (
                xt[z, h].astype(F32)
                + mine[FEAT * h:FEAT * h + FEAT]
                + (cin[0, PAIRS - 1, h].astype(F32) + lin[0, PAIRS - 1, h].astype(F32))
                + (cin[1, PAIRS - 2, h].astype(F32) + lin[1, PAIRS - 1, h].astype(F32))
            )
            if h == 0:
                res[0] = total.astype(BF16)
                remote(res.at[0], res.at[0], res_send, res_recv, partner).start()
            else:
                out_ref[...] = total.astype(BF16)

        remote(xt.at[pl.ds(0, NZ - 1)], xt.at[pl.ds(0, NZ - 1)], ag_send, own_recv, partner).wait_send()
        remote(xt.at[pl.ds(0, 24)], xt.at[pl.ds(0, 24)], y_send, own_recv, partner).wait_send()
        remote(x4, x4, x_send, own_recv, partner).wait_send()
        for n in range(7):
            remote(st.at[y], st.at[y], st_send.at[n], own_recv, partner).wait_send()
        remote(pout.at[pl.ds(0, 3)], pout.at[pl.ds(0, 3)], p_send, own_recv, partner).wait_send()
        for w, ref in ((0, wb), (1, wo)):
            remote(ref, ref, nb_send.at[w], nb_recv.at[w], partner).wait_send()
        for dr, n in ((0, PAIRS), (1, PAIRS - 1)):
            ref = cout.at[dr, pl.ds(0, n)]
            remote(ref, ref, c_send.at[dr], own_recv, partner).wait_send()
            ref = lout.at[dr]
            remote(ref, ref, l_send.at[dr], own_recv, partner).wait_send()
        remote(res.at[0], res.at[0], res_send, res_recv, partner).wait_send()


def body(tokens, norm_gain, hidden_bias, weight_in, weight_out):
    dma = pltpu.SemaphoreType.DMA
    vmem = pl.BlockSpec(memory_space=pltpu.VMEM)
    return pl.pallas_call(
        kernel,
        out_shape=jax.ShapeDtypeStruct((FEAT, TOK), BF16),
        in_specs=[vmem] * 5,
        out_specs=vmem,
        scratch_shapes=[
            pltpu.VMEM((NZ, 2, FEAT, TOK), BF16),
            pltpu.VMEM((NP, 8, 2, FEAT, TOK), BF16),
            pltpu.VMEM((NP, BLK, 2 * TOK), BF16),
            pltpu.VMEM((2, NZ, HALF, BLK), BF16),
            pltpu.VMEM((2, NZ, HALF, BLK), BF16),
            pltpu.VMEM((12, 128, 128), F32),
            pltpu.VMEM((NP, 2, 8, TOK), F32),
            pltpu.VMEM((2, 8, TOK), F32),
            pltpu.VMEM((NP, BLK, TOK), BF16),
            pltpu.VMEM((NP, BLK, TOK), BF16),
            pltpu.VMEM((2, BLK, TOK), BF16),
            pltpu.VMEM((2, PAIRS, 2, FEAT, TOK), BF16),
            pltpu.VMEM((2, PAIRS, 2, FEAT, TOK), BF16),
            pltpu.VMEM((2, PAIRS, 2, FEAT, TOK), BF16),
            pltpu.VMEM((2, PAIRS, 2, FEAT, TOK), BF16),
            pltpu.VMEM((1, FEAT, TOK), BF16),
            pltpu.VMEM((2, HALF, TOK), F32),
            pltpu.VMEM((BLK, TOK), F32),
            pltpu.VMEM((NZ, HALF, TOK), F32),
            pltpu.VMEM((NZ, HALF, TOK), F32),
            dma, dma((2, STEPS + 1, 2)), dma, dma, dma((NP, 8, 2)), dma((7,)), dma((NP,)),
            dma, dma((NP,)), dma, dma,
            dma((2, 2)), dma((2, 2, 20)), dma((2, 2)), dma((2, 2, NR)), dma((2,)), dma((2,)),
            dma, dma((NZ,)), dma((2,)), dma((2, PAIRS, 2)), dma((2,)), dma((2, PAIRS)), dma, dma,
        ],
        compiler_params=pltpu.CompilerParams(
            collective_id=0, has_side_effects=True, vmem_limit_bytes=60 * 1024 * 1024
        ),
    )(
        tokens.T,
        norm_gain.reshape(48, 128),
        hidden_bias.reshape(3, 128),
        weight_in,
        weight_out,
    ).T


def solution(mesh):
    finer = Mesh(mesh.devices.reshape(4, 4, 32, 2), ("rows_0", "rows_1", "mp_0", "mp_1"))
    placed = (P(ROWS, MP), P(), P(MP), P(ROWS, MP), P(MP, ROWS))
    return jax.shard_map(body, mesh=finer, in_specs=placed, out_specs=P(ROWS, MP), check_vma=False)
```
